32 devices in a mesh: dp: 2 (over x), expert: 4 (over z), tensor: 4 (over y, core).
Axes of the slice: x: 2, y: 2, z: 4, core: 2. Of those that a mesh axis runs over, the one named last changes fastest.
Arguments:
- tokens: bfloat16 [1024, 7168], P(('dp', 'expert'), 'tensor'), may hold values from -6 to 6
- expert_ids: int32 [1024, 2], P(('dp', 'expert')), may hold values from 0 to 3, all different within a row; in each aligned block of 128 rows (0 to 127, 128 to 255, ...) at most 96 rows name the same one
- gate_scores: bfloat16 [1024, 2], P(('dp', 'expert')), may hold values from 0.099609375 to 0.59765625
- weight_in: bfloat16 [4, 2, 7168, 1024], P('expert', None, 'tensor', 'dp'), may hold values from -0.0625 to 0.0625
- weight_out: bfloat16 [4, 1024, 7168], P('expert', 'dp', 'tensor'), may hold values from -0.1875 to 0.1875
Outputs:
- mixed: bfloat16 [1024, 7168], P(('dp', 'expert'), 'tensor')
The draws below stay inside these ranges and needn't reach their ends.
Inputs may be any that keep to these rules, and one draw needn't show every extreme that they name: `expert_ids`: each token names 2 different experts; among the 128 tokens of one index of dp and expert together (aligned blocks of rows) no expert is named more than 96 times, and in some blocks an expert is named exactly 96 times.
All inputs are finite; a program needn't handle non-finite values.
Results may differ from the reference program's by a relative error of at most 0.0071.
Values may be sent and summed in bfloat16 or wider, within the bound.
A program may use at most 64 MiB of HBM per device.

```python
import math
import jax
import jax.numpy as jnp
import numpy as np
from jax import lax

D = 7168
FF = 1024
TOK_GRP = 128
TOP = 2
EXPERTS = 4
CAP = 96
TOKENS = 1024


def shard_levels(rng, dims, cuts, low, top_value):
    level = 1.0
    for position, shards_of in cuts:
        heights = jax.random.uniform(jax.random.fold_in(jax.random.fold_in(rng, 6), position), (shards_of,), jnp.float32, low / len(cuts), top_value / len(cuts))
        level = level * jnp.repeat(jnp.exp(heights), dims[position] // shards_of).reshape((-1,) + (1,) * (len(dims) - 1 - position))
    return level


def routed_block(own_key, own, number, rows, count, top, limit, lean):
    order = jax.random.permutation(own_key, count)
    crowded, usual = shares(count, rows * top, limit, lean, True), shares(count, rows * top, limit, lean, False)
    places = jnp.arange(count)

    def named(tallies, offset_by):
        used = int((tallies > 0).sum())
        fixed = max(1, used // 4)
        shifted = fixed + (places - fixed + offset_by * (used - fixed)) % max(1, count - fixed)
        return jnp.zeros((count,), jnp.int32).at[order[jnp.where(places < fixed, places, shifted)]].set(jnp.asarray(tallies, jnp.int32))

    tallies = jnp.where(number % 4 == 0, named(crowded, number // 4), named(usual, number - number // 4 - 1))
    mixed = jax.random.permutation(jax.random.fold_in(own, 3), count)
    giver, sink = mixed[0:count // 2 * 2:2], mixed[1:count // 2 * 2:2]
    slack = jnp.minimum(tallies[giver] - 1, limit - tallies[sink]) // 2
    slack = jnp.where((giver == order[0]) | (sink == order[0]) | (tallies[sink] == 0), 0, jnp.maximum(slack, 0))
    shifted = jax.random.randint(jax.random.fold_in(own, 4), (count // 2,), 0, 1 << 20) % (slack + 1)
    tallies = tallies.at[giver].add(-shifted).at[sink].add(shifted)
    members = jnp.searchsorted(jnp.cumsum(tallies), jnp.arange(rows * top), side="right").astype(jnp.int32)
    table = members.reshape(top, rows).T
    table = table[jax.random.permutation(jax.random.fold_in(own, 1), rows)]
    offset_by = jax.random.randint(jax.random.fold_in(own, 2), (rows, 1), 0, top)
    return jnp.take_along_axis(table, (jnp.arange(top)[None, :] + offset_by) % top, axis=1)


def shares(count, total, most, slope, full):
    portions = [(1 << 20) // math.isqrt(rank ** slope) + 1 for rank in range(1, count + 1)]
    largest = most if full else min(most, max(-(-total // count), total * portions[0] // sum(portions)))
    least = 1 if total - largest >= count - 1 else 0
    holding, spare = [largest] + [least] * (count - 1), total - largest - least * (count - 1)
    while spare > 0:
        movable = [i for i in range(1, count) if holding[i] < largest] or [i for i in range(1, count) if holding[i] < most]
        whole, budget = sum([portions[i] for i in movable]), spare
        for i in movable:
            more = min(most - holding[i], max(1, budget * portions[i] // whole), spare)
            holding[i] = holding[i] + more
            spare = spare - more
    return np.array(holding)


def noise(own_key, shape, width, limit, cuts=(), kind=jnp.bfloat16):
    drawn = width * jax.random.normal(own_key, shape, jnp.float32)
    if cuts:
        drawn = drawn * shard_levels(own_key, shape, cuts, -0.22, 0.18)
    return jnp.clip(drawn, -limit, limit).astype(kind)


def setup_inputs(seed: int = 0) -> dict:
    key_list = jax.random.split(jax.random.key(seed), 6)
    tokens = noise(key_list[0], (TOKENS, D), 1.0, 6.0, ((0, 8), (1, 4)))
    expert_ids_keys = jax.random.split(jax.random.fold_in(key_list[1], 1), TOKENS // TOK_GRP)
    expert_ids_turns = jax.random.permutation(jax.random.fold_in(key_list[1], 3), TOKENS // TOK_GRP)
    expert_ids = jax.vmap(lambda own, number: routed_block(jax.random.fold_in(key_list[1], 2), own, number, TOK_GRP, EXPERTS, TOP, CAP, 1))(expert_ids_keys, expert_ids_turns).reshape((TOKENS, TOP))
    gate_scores = jnp.clip(0.099609375 + 0.49804688 * jax.random.uniform(key_list[2], (TOKENS, TOP), jnp.float32) ** shard_levels(key_list[2], (TOKENS, TOP), ((0, 8),), -0.2, 0.2), 0.099609375, 0.59765625).astype(jnp.bfloat16)
    weight_in = noise(key_list[3], (EXPERTS, 2, D, FF), D ** -0.5, 0.0625, ((0, 4), (2, 4), (3, 2)))
    weight_out = noise(key_list[4], (EXPERTS, FF, D), FF ** -0.5, 0.1875, ((0, 4), (1, 2), (2, 4)))
    return dict(tokens=tokens, expert_ids=expert_ids, gate_scores=gate_scores, weight_in=weight_in, weight_out=weight_out)


def reference(tokens, expert_ids, gate_scores, weight_in, weight_out):
    groups = TOKENS // TOK_GRP
    wide = tokens.astype(jnp.float32)
    mean_square = lax.optimization_barrier(jnp.mean(wide * wide, axis=1, keepdims=True))
    normed = (wide * lax.rsqrt(mean_square + 1e-06)).astype(jnp.bfloat16)
    grouped = normed.reshape(groups, TOK_GRP, D).astype(jnp.float32)
    flat_ids = expert_ids.reshape(groups, TOK_GRP * TOP)
    one_hot = (flat_ids[:, :, None] == jnp.arange(EXPERTS, dtype=jnp.int32)[None, None, :]).astype(jnp.int32)
    earlier = jnp.cumsum(one_hot, axis=1) - one_hot
    slot_pos = lax.optimization_barrier(jnp.sum(earlier * one_hot, axis=2)).astype(jnp.int32)
    slot_range = jnp.arange(CAP, dtype=jnp.int32)
    scores = gate_scores.astype(jnp.float32).reshape(groups, TOK_GRP, TOP, 1)

    def one_expert(totals, inputs):
        expert, gate_up, down = inputs
        matched = (flat_ids == expert)[:, :, None] & (slot_pos[:, :, None] == slot_range[None, None, :])
        matched = matched.astype(jnp.float32).reshape(groups, TOK_GRP, TOP, CAP)
        picked = lax.optimization_barrier(jnp.sum(matched, axis=2))
        gathered = jnp.einsum('gtc,gtd->gcd', picked, grouped).astype(jnp.bfloat16).reshape(groups * CAP, D)
        gate = jnp.dot(gathered, gate_up[0], preferred_element_type=jnp.float32)
        upward = jnp.dot(gathered, gate_up[1], preferred_element_type=jnp.float32)
        hidden = (jax.nn.silu(gate) * upward).astype(jnp.bfloat16)
        result = jnp.dot(hidden, down, preferred_element_type=jnp.float32).astype(jnp.bfloat16)
        result = result.reshape(groups, CAP, D).astype(jnp.float32)
        weights = lax.optimization_barrier(jnp.sum(matched * scores, axis=2))
        return (totals + jnp.einsum('gtc,gcd->gtd', weights, result), None)
    start_total = jnp.zeros((groups, TOK_GRP, D), jnp.float32)
    totals, unused = lax.scan(one_expert, start_total, (jnp.arange(EXPERTS, dtype=jnp.int32), weight_in, weight_out))
    return totals.reshape(TOKENS, D).astype(jnp.bfloat16)
```

```python
import functools

import jax
import jax.numpy as jnp
from jax import lax
from jax.experimental import pallas as pl
from jax.experimental.pallas import tpu as pltpu
from jax.sharding import PartitionSpec as P

MESH = pl.DeviceIdType.MESH
F32 = jnp.float32
BF16 = jnp.bfloat16
SEND, FORWARD, PROJECT, ACTIVATE, EXPAND, COLLECT = range(6)
EXTRA = 16
KINDS = "SFPAEC"
TUNED = (
    "S000", "F000", "S010", "S011", "S001", "F001", "P001", "P000", "F010", "A001",
    "S030", "A000", "S031", "F011", "P100", "P101", "P010", "F030", "S020", "A100",
    "P110", "E000", "A010", "E100", "P030", "F031", "P130", "P011", "A030", "S021",
    "A101", "P031", "A110", "F020", "P111", "A031", "E110", "P131", "E010", "C000",
    "P120", "F021", "P021", "P020", "A111", "A011", "E101", "A130", "A131", "E030",
    "A120", "P121", "E130", "E131", "C010", "E001", "A020", "A121", "E011", "E031",
    "E121", "C030", "A021", "C001", "E111", "E021", "E120", "C031", "C021", "E020",
    "C011", "C020",
)


def dot(a, b):
    return jnp.dot(a, b, preferred_element_type=F32)


def lookup(values, index):
    base = 1 << max(values).bit_length()
    share = 1
    while base ** (share + 1) < 2**31:
        share += 1
    word = 0
    for i in range(0, len(values), share):
        packed = sum(v * base**k for k, v in enumerate(values[i : i + share]))
        word = jnp.where(index // share == i // share, packed, word)
    place, value = lax.rem(index, share), word
    for k in range(1, share):
        value = jnp.where(place == k, word // base**k, value)
    return lax.rem(value, base)


def make_plan(n_dp, chunks, parts):
    if (n_dp, chunks, parts) == (2, 4, 2):
        return [(KINDS.index(c[0]), *map(int, c[1:])) for c in TUNED]
    own = [(0, p) for p in range(parts)]
    offsets = sorted(range(1, chunks), key=lambda o: (o == 1, o))
    far = [(o, p) for o in offsets for p in range(parts)]
    units = own + far
    plan = []
    for o, p in own:
        plan += [(SEND, 0, o, p)]
    plan += [(SEND, 0, o, p) for o, p in far]
    for o, p in own:
        plan += [(FORWARD, 0, o, p)]
    count = len(units)
    for s in range(count + 4):
        if parts <= s + 1 < count:
            plan.append((FORWARD, 0, *units[s + 1]))
        for kind in (PROJECT, ACTIVATE, EXPAND):
            if s < count:
                plan.append((kind, 0, *units[s]))
            if 0 <= s - 1 < count:
                plan += [(kind, h, *units[s - 1]) for h in range(1, n_dp)]
        if 0 <= s - 3 < count:
            plan.append((COLLECT, 0, *units[s - 3]))
    return plan


def kernel(
    sizes,
    plan,
    tokens_hbm,
    ids,
    scores,
    w_in_hbm,
    w_out_hbm,
    mixed,
    tokens,
    w_in,
    w_out,
    slot_t,
    outgoing,
    rows_in,
    part,
    part_in,
    hidden,
    keep,
    down,
    down_in,
    home,
    home_in,
    local_sem,
    sz,
    rz,
    sx,
    rx,
    sp,
    rp,
    sh,
    rh,
    so,
    ro,
    sr,
    rr,
):
    n_dp, n_ex, n_t, cap, group, parts = sizes
    d, e, t = lax.axis_index("dp"), lax.axis_index("expert"), lax.axis_index("tensor")
    chunks = n_ex // group
    piece = cap // parts
    ec, ei = e // group, lax.rem(e, group)
    tok, width = tokens.shape
    top = ids.shape[0]
    units = w_out.shape[0]
    sub = units // n_t
    rows = group * piece
    width_all = width * n_t

    def at(index, step, count):
        return lax.rem(index + step + count, count)

    def copy(src, dst, send, recv, axis, index):
        return pltpu.make_async_remote_copy(
            src_ref=src, dst_ref=dst, send_sem=send, recv_sem=recv,
            device_id={axis: index}, device_id_type=MESH,
        )

    load_tokens = pltpu.make_async_copy(tokens_hbm, tokens, local_sem.at[0])
    load_in = pltpu.make_async_copy(w_in_hbm.at[0], w_in, local_sem.at[1])
    load_out = pltpu.make_async_copy(w_out_hbm.at[0], w_out, local_sem.at[2])
    load_tokens.start()
    barrier = pltpu.get_barrier_semaphore()
    for axis, me, count in (("dp", d, n_dp), ("expert", e, n_ex), ("tensor", t, n_t)):
        for step in range(1, count):
            pl.semaphore_signal(
                barrier, inc=1, device_id={axis: at(me, step, count)}, device_id_type=MESH
            )
    load_in.start()
    load_out.start()

    tok_rows = lax.broadcasted_iota(jnp.int32, (tok, tok), 0)
    tok_lanes = lax.broadcasted_iota(jnp.int32, (tok, tok), 1)
    wide_ex = max(128, n_ex)
    ex_rows = lax.broadcasted_iota(jnp.int32, (wide_ex, tok), 0)
    named_t = ex_rows < 0
    for k in range(top):
        named_t = named_t | (ex_rows == ids[k : k + 1, :])
    count_t = dot(named_t.astype(F32).astype(BF16), (tok_rows < tok_lanes).astype(F32).astype(BF16))
    slot_t[...] = jnp.where(named_t, count_t, -1.0)

    load_tokens.wait()
    pl.semaphore_wait(barrier, n_dp + n_ex + n_t - 3)

    def block(ref, lead, member, p):
        u = (member // group) * parts + p
        if group == 1:
            return ref.at[(*lead, u)]
        return ref.at[(*lead, u, pl.ds(pl.multiple_of(lax.rem(member, group) * piece, piece), piece))]

    def z_copy(expert, p):
        return copy(
            outgoing.at[expert * parts + p], block(rows_in, (0,), e, p),
            sz.at[expert * parts + p], rz.at[e * parts + p], "expert", expert,
        )

    def z_wait(source, p):
        copy(
            outgoing.at[source * parts + p], block(rows_in, (0,), source, p),
            sz.at[source * parts + p], rz.at[source * parts + p], "expert", source,
        ).wait_recv()

    def x_copy(u, hop):
        return copy(
            rows_in.at[0, u], rows_in.at[n_dp - hop, u],
            sx.at[hop, u], rx.at[n_dp - hop, u], "dp", at(d, hop, n_dp),
        )

    def part_copy(h, u, step):
        to = at(t, step, n_t)
        return copy(part.at[h, u, to], part_in.at[h, u, t], sp.at[h, u, step], rp.at[h, u, t], "tensor", to)

    def hidden_copy(h, u, step):
        to = at(t, step, n_t)
        return copy(hidden.at[h, u, t], hidden.at[h, u, t], sh.at[h, u, step], rh.at[h, u, t], "tensor", to)

    def down_copy(h, u):
        return copy(
            down.at[h - 1, u], down_in.at[n_dp - h - 1, u], so.at[h, u], ro.at[n_dp - h, u], "dp", at(d, h, n_dp)
        )

    def home_copy(expert, p):
        return copy(
            block(home, (), expert, p), home_in.at[e * parts + p],
            sr.at[expert * parts + p], rr.at[e * parts + p], "expert", expert,
        )

    def home_wait(source, p):
        copy(
            block(home, (), source, p), home_in.at[source * parts + p],
            sr.at[source * parts + p], rr.at[source * parts + p], "expert", source,
        ).wait_recv()

    piece_rows = lax.broadcasted_iota(jnp.int32, (piece, tok), 0)

    def picked(expert, p):
        want = (piece_rows + p * piece).astype(F32)
        return (want == slot_t[pl.ds(expert, 1), :]).astype(F32)

    def send(q, p):
        for i in range(group):
            expert = q * group + i
            out = dot(picked(expert, p).astype(BF16), tokens[...]).astype(BF16)

            @pl.when(expert != e)
            def _():
                outgoing[expert * parts + p] = out
                z_copy(expert, p).start()

            @pl.when(expert == e)
            def _():
                block(rows_in, (0,), e, p)[...] = out

    def forward(q, p):
        for i in range(group):
            source = q * group + i

            @pl.when(source != e)
            def _():
                z_wait(source, p)

        for hop in range(1, n_dp):
            x_copy(q * parts + p, hop).start()

    diagonal = lax.broadcasted_iota(jnp.int32, (rows, 2 * sub), 0) == lax.broadcasted_iota(jnp.int32, (rows, 2 * sub), 1)
    extra_rows = lax.broadcasted_iota(jnp.int32, (EXTRA, 2 * sub), 0)

    def project(h, u):
        @pl.when(h > 0)
        def _():
            copy(rows_in.at[0, u], rows_in.at[h, u], sx.at[h, u], rx.at[h, u], "dp", at(d, h, n_dp)).wait_recv()

        block_rows = rows_in[h, u]
        wide = block_rows.astype(F32)
        squares = jnp.sum(wide * wide, axis=1, keepdims=True)
        squares = jnp.sum(jnp.where(diagonal, squares, 0.0), axis=0, keepdims=True)
        high = squares.astype(BF16).astype(F32)
        extra = jnp.where(extra_rows == 0, high, jnp.where(extra_rows == 1, squares - high, 0.0)).astype(BF16)
        for to in range(n_t):
            part[h, u, to, rows:, :] = extra
        for g in range(2):
            sums = dot(block_rows, w_in[g]).astype(BF16)
            for to in range(n_t):
                part[h, u, to, :rows, g * sub : (g + 1) * sub] = sums[:, to * sub : (to + 1) * sub]
        for step in range(1, n_t):
            part_copy(h, u, step).start()

    def activate(h, u):
        total = part[h, u, t].astype(F32)
        for step in range(1, n_t):
            s = at(t, step, n_t)
            copy(part.at[h, u, s], part_in.at[h, u, s], sp.at[h, u, step], rp.at[h, u, s], "tensor", s).wait_recv()
            total = total + part_in[h, u, s].astype(F32)
        squares = jnp.sum(total[rows:], axis=0, keepdims=True)
        squares = jnp.sum(jnp.where(diagonal, squares, 0.0), axis=1, keepdims=True)
        total = total[:rows] * lax.rsqrt(squares / width_all + 1e-06)
        gate, up = total[:, :sub], total[:, sub:]
        hidden[h, u, t] = (gate / (1.0 + jnp.exp(-gate)) * up).astype(BF16)
        for step in range(1, n_t):
            hidden_copy(h, u, step).start()

    def expand(h, u):
        for step in range(1, n_t):
            s = at(t, step, n_t)
            copy(hidden.at[h, u, s], hidden.at[h, u, s], sh.at[h, u, step], rh.at[h, u, s], "tensor", s).wait_recv()
        full = jnp.concatenate([hidden[h, u, s] for s in range(n_t)], axis=1)
        result = dot(full, w_out[...])

        @pl.when(h == 0)
        def _():
            keep[u] = result

        @pl.when(h > 0)
        def _():
            down[h - 1, u] = result.astype(BF16)
            down_copy(h, u).start()

    def collect(q, p):
        u = q * parts + p
        total = keep[u]
        for h in range(1, n_dp):
            copy(
                down.at[h - 1, u], down_in.at[h - 1, u], so.at[h, u], ro.at[h, u], "dp", at(d, h, n_dp)
            ).wait_recv()
            total = total + down_in[h - 1, u].astype(F32)
        home[u] = total.astype(BF16)
        for i in range(group):
            expert = q * group + i

            @pl.when(expert != e)
            def _():
                home_copy(expert, p).start()

            @pl.when(expert == e)
            def _():
                home_in[expert * parts + p] = home[u, i * piece : (i + 1) * piece]

    first_project = min(i for i, op in enumerate(plan) if op[0] == PROJECT)
    first_expand = min(i for i, op in enumerate(plan) if op[0] == EXPAND)

    codes = [kind + 8 * (h + n_dp * (p + parts * o)) for kind, h, o, p in plan]

    @pl.loop(0, len(plan))
    def _(step):
        code = lookup(codes, step)
        kind, rest = lax.rem(code, 8), code // 8
        h, rest = lax.rem(rest, n_dp), rest // n_dp
        p, o = lax.rem(rest, parts), rest // parts
        to, q = lax.rem(ec + o, chunks), lax.rem(ec - o + chunks, chunks)
        u = q * parts + p

        @pl.when(kind == SEND)
        def _():
            with SCOPE("send"):
                send(to, p)

        @pl.when(kind == FORWARD)
        def _():
            with SCOPE("forward"):
                forward(q, p)

        @pl.when(kind == PROJECT)
        def _():
            @pl.when(step == first_project)
            def _():
                load_in.wait()

            with SCOPE("project"):
                project(h, u)

        @pl.when(kind == ACTIVATE)
        def _():
            with SCOPE("activate"):
                activate(h, u)

        @pl.when(kind == EXPAND)
        def _():
            @pl.when(step == first_expand)
            def _():
                load_out.wait()

            with SCOPE("expand"):
                expand(h, u)

        @pl.when(kind == COLLECT)
        def _():
            with SCOPE("collect"):
                collect(q, p)

    weights = []
    for expert in range(n_ex):
        score = jnp.zeros((1, tok), F32)
        for k in range(top):
            score = score + jnp.where(ids[k : k + 1, :] == expert, scores[k : k + 1, :].astype(F32), 0.0)
        weights += [picked(expert, p) * score for p in range(parts)]
    combine = jnp.transpose(jnp.concatenate(weights, axis=0)).astype(BF16)

    with SCOPE("homes"):
        @pl.loop(1, n_ex)
        def _(step):
            source = at(e, step, n_ex)
            for p in range(parts):
                home_wait(source, p)

    with SCOPE("mix"):
        mixed[...] = dot(combine, home_in[...].reshape(n_ex * cap, width)).astype(BF16)

    with SCOPE("drain"):
        @pl.loop(1, n_ex)
        def _(step):
            expert = at(e, step, n_ex)
            for p in range(parts):
                z_copy(expert, p).wait_send()
                home_copy(expert, p).wait_send()

        @pl.loop(0, chunks * parts)
        def _(u):
            for hop in range(1, n_dp):
                x_copy(u, hop).wait_send()
                down_copy(hop, u).wait_send()
            for h in range(n_dp):
                for step in range(1, n_t):
                    part_copy(h, u, step).wait_send()
                    hidden_copy(h, u, step).wait_send()


SCOPE = jax.named_scope


def per_device(sizes, tokens, ids, scores, weight_in, weight_out):
    n_dp, n_ex, n_t, cap, group, parts = sizes
    tok, width = tokens.shape
    units = weight_out.shape[1]
    chunks = n_ex // group
    count = chunks * parts
    piece = cap // parts
    rows = group * piece
    plan = make_plan(n_dp, chunks, parts)
    dma = pltpu.SemaphoreType.DMA
    vmem = pl.BlockSpec(memory_space=pltpu.VMEM)
    hbm = pl.BlockSpec(memory_space=pl.ANY)
    return pl.pallas_call(
        functools.partial(kernel, sizes, plan),
        out_shape=jax.ShapeDtypeStruct((tok, width), BF16),
        in_specs=[hbm, vmem, vmem, hbm, hbm],
        out_specs=vmem,
        scratch_shapes=[
            pltpu.VMEM((tok, width), BF16),
            pltpu.VMEM((2, width, units), BF16),
            pltpu.VMEM((units, width), BF16),
            pltpu.VMEM((max(128, n_ex), tok), F32),
            pltpu.VMEM((n_ex * parts, piece, width), BF16),
            pltpu.VMEM((n_dp, count, rows, width), BF16),
            pltpu.VMEM((n_dp, count, n_t, rows + EXTRA, 2 * units // n_t), BF16),
            pltpu.VMEM((n_dp, count, n_t, rows + EXTRA, 2 * units // n_t), BF16),
            pltpu.VMEM((n_dp, count, n_t, rows, units // n_t), BF16),
            pltpu.VMEM((count, rows, width), F32),
            pltpu.VMEM((n_dp - 1, count, rows, width), BF16),
            pltpu.VMEM((n_dp - 1, count, rows, width), BF16),
            pltpu.VMEM((count, rows, width), BF16),
            pltpu.VMEM((n_ex * parts, piece, width), BF16),
            dma((3,)),
            dma((n_ex * parts,)),
            dma((n_ex * parts,)),
            dma((n_dp, count)),
            dma((n_dp, count)),
            dma((n_dp, count, n_t)),
            dma((n_dp, count, n_t)),
            dma((n_dp, count, n_t)),
            dma((n_dp, count, n_t)),
            dma((n_dp, count)),
            dma((n_dp, count)),
            dma((n_ex * parts,)),
            dma((n_ex * parts,)),
        ],
        compiler_params=pltpu.CompilerParams(
            collective_id=0, has_side_effects=True, vmem_limit_bytes=60 * 1024 * 1024
        ),
    )(tokens, ids, scores, weight_in, weight_out)


def solution(mesh):
    n_dp, n_ex, n_t = mesh.shape["dp"], mesh.shape["expert"], mesh.shape["tensor"]

    def whole(tokens, expert_ids, gate_scores, weight_in, weight_out):
        tok = tokens.shape[0] // (n_dp * n_ex)
        slots = min(3 * tok * expert_ids.shape[1] // (2 * n_ex), tok)
        group = max(1, n_ex // n_t)
        parts = 2 if group == 1 else 1
        cap = -(-slots // (16 * parts)) * 16 * parts
        return jax.shard_map(
            functools.partial(per_device, (n_dp, n_ex, n_t, cap, group, parts)),
            mesh=mesh,
            in_specs=(
                P(("dp", "expert"), "tensor"),
                P(None, ("dp", "expert")),
                P(None, ("dp", "expert")),
                P("expert", None, "tensor", "dp"),
                P("expert", "dp", "tensor"),
            ),
            out_specs=P(("dp", "expert"), "tensor"),
            check_vma=False,
        )(tokens, expert_ids.T, gate_scores.T, weight_in, weight_out)

    return whole
```

```python
import functools

import jax
import jax.numpy as jnp
from jax import lax
from jax.experimental import pallas as pl
from jax.experimental.pallas import tpu as pltpu
from jax.sharding import PartitionSpec as P

MESH = pl.DeviceIdType.MESH
F32 = jnp.float32
BF16 = jnp.bfloat16
SEND, FORWARD, PROJECT, ACTIVATE, EXPAND, COLLECT = range(6)
EXTRA = 16
KINDS = "SFPAEC"
TUNED = (
    "S000", "F000", "S010", "S011", "S001", "F001", "P001", "P000", "F010", "A001",
    "S030", "A000", "S031", "F011", "P100", "P101", "P010", "F030", "S020", "A100",
    "P110", "E000", "A010", "E100", "P030", "F031", "P130", "P011", "A030", "S021",
    "A101", "P031", "A110", "F020", "P111", "A031", "E110", "P131", "E010", "C000",
    "P120", "F021", "P021", "P020", "A111", "A011", "E101", "A130", "A131", "E030",
    "A120", "P121", "E130", "E131", "C010", "E001", "A020", "A121", "E011", "E031",
    "E121", "C030", "A021", "C001", "E111", "E021", "E120", "C031", "C021", "E020",
    "C011", "C020",
)


def dot(a, b):
    return jnp.dot(a, b, preferred_element_type=F32)


def lookup(values, index):
    base = 1 << max(values).bit_length()
    share = 1
    while base ** (share + 1) < 2**31:
        share += 1
    word = 0
    for i in range(0, len(values), share):
        packed = sum(v * base**k for k, v in enumerate(values[i : i + share]))
        word = jnp.where(index // share == i // share, packed, word)
    place, value = lax.rem(index, share), word
    for k in range(1, share):
        value = jnp.where(place == k, word // base**k, value)
    return lax.rem(value, base)


def make_plan(n_dp, chunks, parts):
    if (n_dp, chunks, parts) == (2, 4, 2):
        return [(KINDS.index(c[0]), *map(int, c[1:])) for c in TUNED]
    own = [(0, p) for p in range(parts)]
    offsets = sorted(range(1, chunks), key=lambda o: (o == 1, o))
    far = [(o, p) for o in offsets for p in range(parts)]
    units = own + far
    plan = []
    for o, p in own:
        plan += [(SEND, 0, o, p)]
    plan += [(SEND, 0, o, p) for o, p in far]
    for o, p in own:
        plan += [(FORWARD, 0, o, p)]
    count = len(units)
    for s in range(count + 4):
        if parts <= s + 1 < count:
            plan.append((FORWARD, 0, *units[s + 1]))
        for kind in (PROJECT, ACTIVATE, EXPAND):
            if s < count:
                plan.append((kind, 0, *units[s]))
            if 0 <= s - 1 < count:
                plan += [(kind, h, *units[s - 1]) for h in range(1, n_dp)]
        if 0 <= s - 3 < count:
            plan.append((COLLECT, 0, *units[s - 3]))
    return plan


def kernel(
    sizes,
    plan,
    tokens_hbm,
    ids,
    scores,
    w_in_hbm,
    w_out_hbm,
    mixed,
    tokens,
    w_in,
    w_out,
    slot_t,
    outgoing,
    rows_in,
    part,
    part_in,
    hidden,
    keep,
    down,
    down_in,
    home,
    home_in,
    local_sem,
    sz,
    rz,
    sx,
    rx,
    sp,
    rp,
    sh,
    rh,
    so,
    ro,
    sr,
    rr,
):
    n_dp, n_ex, n_t, cap, group, parts = sizes
    d, e, t = lax.axis_index("dp"), lax.axis_index("expert"), lax.axis_index("tensor")
    chunks = n_ex // group
    piece = cap // parts
    ec, ei = e // group, lax.rem(e, group)
    tok, width = tokens.shape
    top = ids.shape[0]
    units = w_out.shape[0]
    sub = units // n_t
    rows = group * piece
    width_all = width * n_t

    def at(index, step, count):
        return lax.rem(index + step + count, count)

    def copy(src, dst, send, recv, axis, index):
        return pltpu.make_async_remote_copy(
            src_ref=src, dst_ref=dst, send_sem=send, recv_sem=recv,
            device_id={axis: index}, device_id_type=MESH,
        )

    def pending(like, sem):
        return pltpu.make_async_copy(like, like, sem)

    load_tokens = pltpu.make_async_copy(tokens_hbm, tokens, local_sem.at[0])
    load_in = pltpu.make_async_copy(w_in_hbm.at[0], w_in, local_sem.at[1])
    load_out = pltpu.make_async_copy(w_out_hbm.at[0], w_out, local_sem.at[2])
    load_tokens.start()
    barrier = pltpu.get_barrier_semaphore()
    for axis, me, count in (("dp", d, n_dp), ("expert", e, n_ex), ("tensor", t, n_t)):
        for step in range(1, count):
            pl.semaphore_signal(
                barrier, inc=1, device_id={axis: at(me, step, count)}, device_id_type=MESH
            )
    load_in.start()
    load_out.start()

    tok_rows = lax.broadcasted_iota(jnp.int32, (tok, tok), 0)
    tok_lanes = lax.broadcasted_iota(jnp.int32, (tok, tok), 1)
    wide_ex = max(128, n_ex)
    ex_rows = lax.broadcasted_iota(jnp.int32, (wide_ex, tok), 0)
    named_t = ex_rows < 0
    for k in range(top):
        named_t = named_t | (ex_rows == ids[k : k + 1, :])
    count_t = dot(named_t.astype(F32).astype(BF16), (tok_rows < tok_lanes).astype(F32).astype(BF16))
    slot_t[...] = jnp.where(named_t, count_t, -1.0)

    load_tokens.wait()
    pl.semaphore_wait(barrier, n_dp + n_ex + n_t - 3)

    def block(ref, lead, member, p):
        u = (member // group) * parts + p
        if group == 1:
            return ref.at[(*lead, u)]
        return ref.at[(*lead, u, pl.ds(pl.multiple_of(lax.rem(member, group) * piece, piece), piece))]

    def z_copy(expert, p):
        return copy(
            outgoing.at[expert * parts + p], block(rows_in, (0,), e, p),
            sz, rz.at[e * parts + p], "expert", expert,
        )

    def z_wait(source, p):
        copy(
            outgoing.at[source * parts + p], block(rows_in, (0,), source, p),
            sz, rz.at[source * parts + p], "expert", source,
        ).wait_recv()

    def x_copy(u, hop):
        return copy(
            rows_in.at[0, u], rows_in.at[n_dp - hop, u],
            sx, rx.at[n_dp - hop - 1, u], "dp", at(d, hop, n_dp),
        )

    def part_copy(h, u, step):
        to = at(t, step, n_t)
        return copy(part.at[h, u, to], part_in.at[h, u, t], sp, rp.at[h, u], "tensor", to)

    def hidden_copy(h, u, step):
        to = at(t, step, n_t)
        return copy(hidden.at[h, u, t], hidden.at[h, u, t], sh, rh.at[h, u], "tensor", to)

    def down_copy(h, u):
        return copy(
            down.at[h - 1, u], down_in.at[n_dp - h - 1, u], so, ro.at[n_dp - h - 1, u], "dp", at(d, h, n_dp)
        )

    def home_copy(expert, p):
        return copy(
            block(home, (), expert, p), home_in.at[e * parts + p],
            sr, rr, "expert", expert,
        )

    piece_rows = lax.broadcasted_iota(jnp.int32, (piece, tok), 0)

    def picked(expert, p):
        want = (piece_rows + p * piece).astype(F32)
        return (want == slot_t[pl.ds(expert, 1), :]).astype(F32)

    def send(q, p):
        for i in range(group):
            expert = q * group + i
            out = dot(picked(expert, p).astype(BF16), tokens[...]).astype(BF16)

            @pl.when(expert != e)
            def _():
                outgoing[expert * parts + p] = out
                z_copy(expert, p).start()

            @pl.when(expert == e)
            def _():
                block(rows_in, (0,), e, p)[...] = out

    def forward(q, p):
        for i in range(group):
            source = q * group + i

            @pl.when(source != e)
            def _():
                z_wait(source, p)

        for hop in range(1, n_dp):
            x_copy(q * parts + p, hop).start()

    diagonal = lax.broadcasted_iota(jnp.int32, (rows, 2 * sub), 0) == lax.broadcasted_iota(jnp.int32, (rows, 2 * sub), 1)
    extra_rows = lax.broadcasted_iota(jnp.int32, (EXTRA, 2 * sub), 0)

    def project(h, u):
        @pl.when(h > 0)
        def _():
            copy(rows_in.at[0, u], rows_in.at[h, u], sx, rx.at[h - 1, u], "dp", at(d, h, n_dp)).wait_recv()

        block_rows = rows_in[h, u]
        wide = block_rows.astype(F32)
        squares = jnp.sum(wide * wide, axis=1, keepdims=True)
        squares = jnp.sum(jnp.where(diagonal, squares, 0.0), axis=0, keepdims=True)
        high = squares.astype(BF16).astype(F32)
        extra = jnp.where(extra_rows == 0, high, jnp.where(extra_rows == 1, squares - high, 0.0)).astype(BF16)
        for to in range(n_t):
            part[h, u, to, rows:, :] = extra
        for g in range(2):
            sums = dot(block_rows, w_in[g]).astype(BF16)
            for to in range(n_t):
                part[h, u, to, :rows, g * sub : (g + 1) * sub] = sums[:, to * sub : (to + 1) * sub]
        for step in range(1, n_t):
            part_copy(h, u, step).start()

    def activate(h, u):
        pending(part_in.at[h, u, : n_t - 1], rp.at[h, u]).wait()
        total = part[h, u, t].astype(F32)
        for step in range(1, n_t):
            total = total + part_in[h, u, at(t, step, n_t)].astype(F32)
        squares = jnp.sum(total[rows:], axis=0, keepdims=True)
        squares = jnp.sum(jnp.where(diagonal, squares, 0.0), axis=1, keepdims=True)
        total = total[:rows] * lax.rsqrt(squares / width_all + 1e-06)
        gate, up = total[:, :sub], total[:, sub:]
        hidden[h, u, t] = (gate / (1.0 + jnp.exp(-gate)) * up).astype(BF16)
        for step in range(1, n_t):
            hidden_copy(h, u, step).start()

    def expand(h, u):
        pending(hidden.at[h, u, : n_t - 1], rh.at[h, u]).wait()
        full = jnp.concatenate([hidden[h, u, s] for s in range(n_t)], axis=1)
        result = dot(full, w_out[...])

        @pl.when(h == 0)
        def _():
            keep[u] = result

        @pl.when(h > 0)
        def _():
            down[h - 1, u] = result.astype(BF16)
            down_copy(h, u).start()

    def collect(q, p):
        u = q * parts + p
        total = keep[u]
        for h in range(1, n_dp):
            copy(
                down.at[h - 1, u], down_in.at[h - 1, u], so, ro.at[h - 1, u], "dp", at(d, h, n_dp)
            ).wait_recv()
            total = total + down_in[h - 1, u].astype(F32)
        home[u] = total.astype(BF16)
        for i in range(group):
            expert = q * group + i

            @pl.when(expert != e)
            def _():
                home_copy(expert, p).start()

            @pl.when(expert == e)
            def _():
                home_in[expert * parts + p] = home[u, i * piece : (i + 1) * piece]

    first_project = min(i for i, op in enumerate(plan) if op[0] == PROJECT)
    first_expand = min(i for i, op in enumerate(plan) if op[0] == EXPAND)

    codes = [kind + 8 * (h + n_dp * (p + parts * o)) for kind, h, o, p in plan]

    @pl.loop(0, len(plan))
    def _(step):
        code = lookup(codes, step)
        kind, rest = lax.rem(code, 8), code // 8
        h, rest = lax.rem(rest, n_dp), rest // n_dp
        p, o = lax.rem(rest, parts), rest // parts
        to, q = lax.rem(ec + o, chunks), lax.rem(ec - o + chunks, chunks)
        u = q * parts + p

        @pl.when(kind == SEND)
        def _():
            with SCOPE("send"):
                send(to, p)

        @pl.when(kind == FORWARD)
        def _():
            with SCOPE("forward"):
                forward(q, p)

        @pl.when(kind == PROJECT)
        def _():
            @pl.when(step == first_project)
            def _():
                load_in.wait()

            with SCOPE("project"):
                project(h, u)

        @pl.when(kind == ACTIVATE)
        def _():
            with SCOPE("activate"):
                activate(h, u)

        @pl.when(kind == EXPAND)
        def _():
            @pl.when(step == first_expand)
            def _():
                load_out.wait()

            with SCOPE("expand"):
                expand(h, u)

        @pl.when(kind == COLLECT)
        def _():
            with SCOPE("collect"):
                collect(q, p)

    weights = []
    for expert in range(n_ex):
        score = jnp.zeros((1, tok), F32)
        for k in range(top):
            score = score + jnp.where(ids[k : k + 1, :] == expert, scores[k : k + 1, :].astype(F32), 0.0)
        weights += [picked(expert, p) * score for p in range(parts)]
    combine = jnp.transpose(jnp.concatenate(weights, axis=0)).astype(BF16)

    others = (n_ex - 1) * parts
    with SCOPE("homes"):
        pending(home_in.at[:others], rr).wait()

    with SCOPE("mix"):
        mixed[...] = dot(combine, home_in[...].reshape(n_ex * cap, width)).astype(BF16)

    with SCOPE("drain"):
        pending(outgoing.at[:others], sz).wait()
        pending(home_in.at[:others], sr).wait()
        pending(down, so).wait()
        pending(rows_in.at[1:], sx).wait()
        pending(part.at[:, :, : n_t - 1], sp).wait()
        pending(hidden.at[:, :, : n_t - 1], sh).wait()


SCOPE = jax.named_scope


def per_device(sizes, tokens, ids, scores, weight_in, weight_out):
    n_dp, n_ex, n_t, cap, group, parts = sizes
    tok, width = tokens.shape
    units = weight_out.shape[1]
    chunks = n_ex // group
    count = chunks * parts
    piece = cap // parts
    rows = group * piece
    plan = make_plan(n_dp, chunks, parts)
    dma = pltpu.SemaphoreType.DMA
    vmem = pl.BlockSpec(memory_space=pltpu.VMEM)
    hbm = pl.BlockSpec(memory_space=pl.ANY)
    return pl.pallas_call(
        functools.partial(kernel, sizes, plan),
        out_shape=jax.ShapeDtypeStruct((tok, width), BF16),
        in_specs=[hbm, vmem, vmem, hbm, hbm],
        out_specs=vmem,
        scratch_shapes=[
            pltpu.VMEM((tok, width), BF16),
            pltpu.VMEM((2, width, units), BF16),
            pltpu.VMEM((units, width), BF16),
            pltpu.VMEM((max(128, n_ex), tok), F32),
            pltpu.VMEM((n_ex * parts, piece, width), BF16),
            pltpu.VMEM((n_dp, count, rows, width), BF16),
            pltpu.VMEM((n_dp, count, n_t, rows + EXTRA, 2 * units // n_t), BF16),
            pltpu.VMEM((n_dp, count, n_t, rows + EXTRA, 2 * units // n_t), BF16),
            pltpu.VMEM((n_dp, count, n_t, rows, units // n_t), BF16),
            pltpu.VMEM((count, rows, width), F32),
            pltpu.VMEM((n_dp - 1, count, rows, width), BF16),
            pltpu.VMEM((n_dp - 1, count, rows, width), BF16),
            pltpu.VMEM((count, rows, width), BF16),
            pltpu.VMEM((n_ex * parts, piece, width), BF16),
            dma((3,)),
            dma,
            dma((n_ex * parts,)),
            dma,
            dma((n_dp - 1, count)),
            dma,
            dma((n_dp, count)),
            dma,
            dma((n_dp, count)),
            dma,
            dma((n_dp - 1, count)),
            dma,
            dma,
        ],
        compiler_params=pltpu.CompilerParams(
            collective_id=0, has_side_effects=True, vmem_limit_bytes=60 * 1024 * 1024
        ),
    )(tokens, ids, scores, weight_in, weight_out)


def solution(mesh):
    n_dp, n_ex, n_t = mesh.shape["dp"], mesh.shape["expert"], mesh.shape["tensor"]

    def whole(tokens, expert_ids, gate_scores, weight_in, weight_out):
        tok = tokens.shape[0] // (n_dp * n_ex)
        slots = min(3 * tok * expert_ids.shape[1] // (2 * n_ex), tok)
        group = max(1, n_ex // n_t)
        parts = 2 if group == 1 else 1
        cap = -(-slots // (16 * parts)) * 16 * parts
        return jax.shard_map(
            functools.partial(per_device, (n_dp, n_ex, n_t, cap, group, parts)),
            mesh=mesh,
            in_specs=(
                P(("dp", "expert"), "tensor"),
                P(None, ("dp", "expert")),
                P(None, ("dp", "expert")),
                P("expert", None, "tensor", "dp"),
                P("expert", "dp", "tensor"),
            ),
            out_specs=P(("dp", "expert"), "tensor"),
            check_vma=False,
        )(tokens, expert_ids.T, gate_scores.T, weight_in, weight_out)

    return whole
```

```python
import functools

import jax
import jax.numpy as jnp
from jax import lax
from jax.experimental import pallas as pl
from jax.experimental.pallas import tpu as pltpu
from jax.sharding import PartitionSpec as P

MESH = pl.DeviceIdType.MESH
F32 = jnp.float32
BF16 = jnp.bfloat16
SEND, FORWARD, PROJECT, ACTIVATE, EXPAND, COLLECT = range(6)
KINDS = "SFPAEC"
TUNED = (
    "S011", "F001", "P001", "S012", "F002", "P000", "P002", "S031", "F011", "S030", "S032", "P011",
    "F012", "P102", "F031", "S020", "P012", "P031", "P101", "S022", "F000", "P112", "F030", "P111",
    "P131", "A012", "F032", "A111", "A131", "F020", "A112", "S021", "P100", "P020", "S010", "F022",
    "A031", "P132", "A011", "A002", "E112", "E111", "P120", "P032", "P122", "P022", "E012", "E131",
    "C012", "A020", "A120", "A132", "A032", "F021", "E011", "A122", "C011", "E031", "P021", "A022",
    "A001", "E020", "C031", "E122", "E032", "F010", "E120", "P121", "E022", "P130", "C022", "P010",
    "A021", "E132", "A121", "P110", "A130", "P030", "C020", "E121", "A110", "A010", "E001", "A100",
    "E130", "A030", "C032", "A101", "A000", "E021", "C021", "E110", "E010", "A102", "E030", "E101",
    "E100", "C030", "E102", "C010", "E002", "E000", "C000", "C001", "C002",
)


def dot(a, b):
    return jnp.dot(a, b, preferred_element_type=F32)


def lookup(values, index):
    base = 1 << max(values).bit_length()
    share = 1
    while base ** (share + 1) < 2**31:
        share += 1
    word = 0
    for i in range(0, len(values), share):
        packed = sum(v * base**k for k, v in enumerate(values[i : i + share]))
        word = jnp.where(index // share == i // share, packed, word)
    place, value = lax.rem(index, share), word
    for k in range(1, share):
        value = jnp.where(place == k, word // base**k, value)
    return lax.rem(value, base)


def make_plan(n_dp, chunks, parts):
    if (n_dp, chunks, parts) == (2, 4, 3):
        return [(KINDS.index(c[0]), *map(int, c[1:])) for c in TUNED]
    own = [(0, p) for p in range(parts)]
    offsets = sorted(range(1, chunks), key=lambda o: (o == 1, o))
    far = [(o, p) for o in offsets for p in range(parts)]
    units = own + far
    plan = []
    plan += [(SEND, 0, o, p) for o, p in far]
    for o, p in own:
        plan += [(FORWARD, 0, o, p)]
    count = len(units)
    for s in range(count + 4):
        if parts <= s + 1 < count:
            plan.append((FORWARD, 0, *units[s + 1]))
        for kind in (PROJECT, ACTIVATE, EXPAND):
            if s < count:
                plan.append((kind, 0, *units[s]))
            if 0 <= s - 1 < count:
                plan += [(kind, h, *units[s - 1]) for h in range(1, n_dp)]
        if 0 <= s - 3 < count:
            plan.append((COLLECT, 0, *units[s - 3]))
    return plan


def kernel(
    sizes,
    plan,
    tokens_hbm,
    ids_hbm,
    scores_hbm,
    w_in_hbm,
    w_out_hbm,
    mixed,
    tokens,
    ids,
    scores,
    w_in,
    w_out,
    slot_t,
    squares,
    scale_out,
    scales_in,
    outgoing,
    rows_in,
    part,
    part_in,
    hidden,
    keep,
    down,
    down_in,
    home,
    home_in,
    result,
    local_sem,
    sq,
    rq,
    sn,
    sm,
    rn,
    sz,
    rz,
    sx,
    rx,
    sp,
    rp,
    sh,
    rh,
    so,
    ro,
    sr,
    rr,
):
    n_dp, n_ex, n_t, cap, group, parts = sizes
    d, e, t = lax.axis_index("dp"), lax.axis_index("expert"), lax.axis_index("tensor")
    chunks = n_ex // group
    piece = cap // parts
    ec, ei = e // group, lax.rem(e, group)
    tok, width = tokens.shape
    top = ids.shape[0]
    units = w_out.shape[0]
    sub = units // n_t
    rows = group * piece
    width_all = width * n_t

    def at(index, step, count):
        return lax.rem(index + step + count, count)

    def copy(src, dst, send, recv, **index):
        return pltpu.make_async_remote_copy(
            src_ref=src, dst_ref=dst, send_sem=send, recv_sem=recv,
            device_id=index, device_id_type=MESH,
        )

    def pending(like, sem):
        return pltpu.make_async_copy(like, like, sem)

    load_tokens = pltpu.make_async_copy(tokens_hbm, tokens, local_sem.at[0])
    load_in = pltpu.make_async_copy(w_in_hbm.at[0], w_in, local_sem.at[1])
    load_out = pltpu.make_async_copy(w_out_hbm.at[0], w_out, local_sem.at[2])
    load_ids = pltpu.make_async_copy(ids_hbm, ids, local_sem.at[3])
    load_scores = pltpu.make_async_copy(scores_hbm, scores, local_sem.at[4])
    load_ids.start()
    load_tokens.start()
    barrier = pltpu.get_barrier_semaphore()
    for axis, me, count in (("expert", e, n_ex), ("dp", d, n_dp), ("tensor", t, n_t)):
        for step in range(1, count):
            pl.semaphore_signal(
                barrier, inc=1, device_id={axis: at(me, step, count)}, device_id_type=MESH
            )
    load_scores.start()
    load_in.start()
    load_out.start()

    tok_rows = lax.broadcasted_iota(jnp.int32, (tok, tok), 0)
    tok_lanes = lax.broadcasted_iota(jnp.int32, (tok, tok), 1)
    wide_ex = max(128, n_ex)
    ex_rows = lax.broadcasted_iota(jnp.int32, (wide_ex, tok), 0)
    named_t = ex_rows < 0
    load_ids.wait()
    for k in range(top):
        named_t = named_t | (ex_rows == ids[k : k + 1, :])
    count_t = dot(named_t.astype(F32).astype(BF16), (tok_rows < tok_lanes).astype(F32).astype(BF16))
    slot_t[...] = jnp.where(named_t, count_t, -1.0)

    def block(ref, lead, member, p):
        u = (member // group) * parts + p
        if group == 1:
            return ref.at[(*lead, u)]
        return ref.at[(*lead, u, pl.ds(pl.multiple_of(lax.rem(member, group) * piece, piece), piece))]

    def z_copy(expert, p):
        return copy(
            outgoing.at[expert * parts + p], block(rows_in, (0,), e, p),
            sz, rz.at[e * parts + p], expert=expert,
        )

    def z_wait(source, p):
        copy(
            outgoing.at[source * parts + p], block(rows_in, (0,), source, p),
            sz, rz.at[source * parts + p], expert=source,
        ).wait_recv()

    def x_copy(u, hop):
        return copy(
            rows_in.at[0, u], rows_in.at[n_dp - hop, u],
            sx, rx.at[n_dp - hop - 1, u], dp=at(d, hop, n_dp),
        )

    def part_copy(h, u, step):
        to = at(t, step, n_t)
        return copy(part.at[h, u, to], part_in.at[h, u, t], sp, rp.at[h, u], tensor=to)

    def hidden_copy(h, u, step):
        to = at(t, step, n_t)
        return copy(hidden.at[h, u, t], hidden.at[h, u, t], sh, rh.at[h, u], tensor=to)

    def down_copy(h, u):
        return copy(
            down.at[h - 1, u], down_in.at[n_dp - h - 1, u], so, ro.at[n_dp - h - 1, u], dp=at(d, h, n_dp)
        )

    def home_copy(expert, p):
        return copy(
            block(home, (), expert, p), home_in.at[e * parts + p],
            sr, rr, expert=expert,
        )

    piece_rows = lax.broadcasted_iota(jnp.int32, (piece, tok), 0)
    diagonal = piece_rows == lax.broadcasted_iota(jnp.int32, (piece, tok), 1)

    def picked(expert, p):
        want = (piece_rows + p * piece).astype(F32)
        return want == slot_t[expert : expert + 1, :]

    with SCOPE("tok"):
        load_tokens.wait()
    for expert in range(n_ex):
        pick = jnp.concatenate([picked(expert, p).astype(F32) for p in range(parts)], axis=0).astype(BF16)
        outgoing[expert * parts : (expert + 1) * parts] = (
            dot(pick, tokens[...]).astype(BF16).reshape(parts, piece, width)
        )
    for p in range(parts):
        block(rows_in, (0,), e, p)[...] = outgoing[e * parts + p]
    wide = tokens[...].astype(F32)
    own_squares = jnp.sum(wide * wide, axis=1, keepdims=True)
    own_squares = jnp.sum(jnp.where(tok_rows == tok_lanes, own_squares, 0.0), axis=0, keepdims=True)
    squares[t] = jnp.broadcast_to(own_squares, (8, tok))
    with SCOPE("barrier"):
        pl.semaphore_wait(barrier, n_dp + n_ex + n_t - 3)
    for step in range(1, n_t):
        copy(squares.at[t], squares.at[t], sq, rq, tensor=at(t, step, n_t)).start()

    def normalize():
        pending(squares.at[: n_t - 1], rq).wait()
        total = squares[0, 0:1, :]
        for s in range(1, n_t):
            total = total + squares[s, 0:1, :]
        scale = lax.rsqrt(total / width_all + 1e-06)
        tile_rows = lax.broadcasted_iota(jnp.int32, (8, tok), 0)
        for expert in range(n_ex):
            tile = jnp.zeros((8, tok), F32)
            for p in range(parts):
                column = jnp.sum(jnp.where(picked(expert, p), scale, 0.0), axis=1, keepdims=True)
                row = jnp.sum(jnp.where(diagonal, column, 0.0), axis=0, keepdims=True)
                tile = jnp.where(tile_rows == p, row, tile)
            scale_out[expert] = tile
        scales_in[0, e] = scale_out[e]
        for step in range(1, n_ex):
            to = at(e, step, n_ex)
            copy(scale_out.at[to], scales_in.at[0, e], sn, rn.at[0], expert=to).start()

    def spread():
        pending(scales_in.at[0, : n_ex - 1], rn.at[0]).wait()
        for hop in range(1, n_dp):
            copy(scales_in.at[0], scales_in.at[n_dp - hop], sm, rn.at[n_dp - hop], dp=at(d, hop, n_dp)).start()

    def send(q, p):
        for i in range(group):
            expert = q * group + i

            @pl.when(expert != e)
            def _():
                z_copy(expert, p).start()

    def forward(q, p):
        for i in range(group):
            source = q * group + i

            @pl.when(source != e)
            def _():
                z_wait(source, p)

        for hop in range(1, n_dp):
            x_copy(q * parts + p, hop).start()

    def project(h, u):
        @pl.when(h > 0)
        def _():
            copy(rows_in.at[0, u], rows_in.at[h, u], sx, rx.at[h - 1, u], dp=at(d, h, n_dp)).wait_recv()

        block_rows = rows_in[h, u]
        for g in range(2):
            sums = dot(block_rows, w_in[g]).astype(BF16)
            for to in range(n_t):
                part[h, u, to, :, g * sub : (g + 1) * sub] = sums[:, to * sub : (to + 1) * sub]
        for step in range(1, n_t):
            part_copy(h, u, step).start()

    def activate(h, q, p):
        u = q * parts + p
        pending(part_in.at[h, u, : n_t - 1], rp.at[h, u]).wait()
        total = part[h, u, t].astype(F32)
        for step in range(1, n_t):
            total = total + part_in[h, u, at(t, step, n_t)].astype(F32)
        scale = [
            jnp.sum(
                jnp.where(diagonal, scales_in[h, q * group + i, pl.ds(p, 1), :], 0.0), axis=1, keepdims=True
            )
            for i in range(group)
        ]
        total = total * jnp.concatenate(scale, axis=0)
        gate, up = total[:, :sub], total[:, sub:]
        hidden[h, u, t] = (gate / (1.0 + jnp.exp(-gate)) * up).astype(BF16)
        for step in range(1, n_t):
            hidden_copy(h, u, step).start()

    def expand(h, u):
        pending(hidden.at[h, u, : n_t - 1], rh.at[h, u]).wait()
        full = jnp.concatenate([hidden[h, u, s] for s in range(n_t)], axis=1)
        result = dot(full, w_out[...])

        @pl.when(h == 0)
        def _():
            keep[u] = result

        @pl.when(h > 0)
        def _():
            down[h - 1, u] = result.astype(BF16)
            down_copy(h, u).start()

    def collect(q, p):
        u = q * parts + p
        total = keep[u]
        for h in range(1, n_dp):
            copy(
                down.at[h - 1, u], down_in.at[h - 1, u], so, ro.at[h - 1, u], dp=at(d, h, n_dp)
            ).wait_recv()
            total = total + down_in[h - 1, u].astype(F32)
        home[u] = total.astype(BF16)
        for i in range(group):
            expert = q * group + i

            @pl.when(expert != e)
            def _():
                home_copy(expert, p).start()

            @pl.when(expert == e)
            def _():
                home_in[expert * parts + p] = home[u, i * piece : (i + 1) * piece]

    first_project = min(i for i, op in enumerate(plan) if op[0] == PROJECT)
    first_activate = min(i for i, op in enumerate(plan) if op[0] == ACTIVATE)
    first_far_activate = [min(i for i, op in enumerate(plan) if op[:2] == (ACTIVATE, h)) for h in range(1, n_dp)]
    first_far = min(i for i, op in enumerate(plan) if op[0] in (FORWARD, ACTIVATE) and op[2] + (op[0] == ACTIVATE) > 0)
    first_expand = min(i for i, op in enumerate(plan) if op[0] == EXPAND)

    codes = [kind + 8 * (h + n_dp * (p + parts * o)) for kind, h, o, p in plan]

    @pl.loop(0, len(plan))
    def _(step):
        @pl.when(step == first_far)
        def _():
            with SCOPE("normalize"):
                normalize()

        code = lookup(codes, step)
        kind, rest = lax.rem(code, 8), code // 8
        h, rest = lax.rem(rest, n_dp), rest // n_dp
        p, o = lax.rem(rest, parts), rest // parts
        to, q = lax.rem(ec + o, chunks), lax.rem(ec - o + chunks, chunks)
        u = q * parts + p

        @pl.when(kind == SEND)
        def _():
            with SCOPE("send"):
                send(to, p)

        @pl.when(kind == FORWARD)
        def _():
            with SCOPE("forward"):
                forward(q, p)

        @pl.when(kind == PROJECT)
        def _():
            @pl.when(step == first_project)
            def _():
                load_in.wait()

            with SCOPE("project"):
                project(h, u)

        @pl.when(kind == ACTIVATE)
        def _():
            @pl.when(step == first_activate)
            def _():
                spread()

            for hop in range(1, n_dp):
                @pl.when(step == first_far_activate[hop - 1])
                def _():
                    pending(scales_in.at[hop], rn.at[hop]).wait()

            with SCOPE("activate"):
                activate(h, q, p)

        @pl.when(kind == EXPAND)
        def _():
            @pl.when(step == first_expand)
            def _():
                load_out.wait()

            with SCOPE("expand"):
                expand(h, u)

        @pl.when(kind == COLLECT)
        def _():
            with SCOPE("collect"):
                collect(q, p)

    load_scores.wait()
    weights = []
    for expert in range(n_ex):
        score = jnp.zeros((1, tok), F32)
        for k in range(top):
            score = score + jnp.where(ids[k : k + 1, :] == expert, scores[k : k + 1, :].astype(F32), 0.0)
        weights += [jnp.where(picked(expert, p), score, 0.0) for p in range(parts)]
    combine = jnp.transpose(jnp.concatenate(weights, axis=0)).astype(BF16)

    others = (n_ex - 1) * parts
    with SCOPE("homes"):
        pending(home_in.at[:others], rr).wait()

    stores = []
    with SCOPE("mix"):
        for i, start in enumerate(range(0, width, width // 2)):
            columns = slice(start, start + width // 2)
            result[:, columns] = dot(combine, home_in[:, :, columns].reshape(n_ex * cap, width // 2)).astype(BF16)
            stores.append(pltpu.make_async_copy(result.at[:, columns], mixed.at[:, columns], local_sem.at[i]))
            stores[i].start()

    with SCOPE("drain"):
        pending(squares.at[: n_t - 1], sq).wait()
        pending(scales_in.at[0, : n_ex - 1], sn).wait()
        pending(scales_in.at[1:], sm).wait()
        pending(outgoing.at[:others], sz).wait()
        pending(home_in.at[:others], sr).wait()
        pending(down, so).wait()
        pending(rows_in.at[1:], sx).wait()
        pending(part.at[:, :, : n_t - 1], sp).wait()
        pending(hidden.at[:, :, : n_t - 1], sh).wait()
        for store in stores:
            store.wait()


SCOPE = jax.named_scope


def per_device(sizes, tokens, ids, scores, weight_in, weight_out):
    n_dp, n_ex, n_t, cap, group, parts = sizes
    tok, width = tokens.shape
    units = weight_out.shape[1]
    chunks = n_ex // group
    count = chunks * parts
    piece = cap // parts
    rows = group * piece
    plan = make_plan(n_dp, chunks, parts)
    dma = pltpu.SemaphoreType.DMA
    top = ids.shape[0]
    hbm = pl.BlockSpec(memory_space=pl.ANY)
    return pl.pallas_call(
        functools.partial(kernel, sizes, plan),
        out_shape=jax.ShapeDtypeStruct((tok, width), BF16),
        in_specs=[hbm] * 5,
        out_specs=hbm,
        scratch_shapes=[
            pltpu.VMEM((tok, width), BF16),
            pltpu.VMEM((top, tok), jnp.int32),
            pltpu.VMEM((top, tok), BF16),
            pltpu.VMEM((2, width, units), BF16),
            pltpu.VMEM((units, width), BF16),
            pltpu.VMEM((max(128, n_ex), tok), F32),
            pltpu.VMEM((n_t, 8, tok), F32),
            pltpu.VMEM((n_ex, 8, tok), F32),
            pltpu.VMEM((n_dp, n_ex, 8, tok), F32),
            pltpu.VMEM((n_ex * parts, piece, width), BF16),
            pltpu.VMEM((n_dp, count, rows, width), BF16),
            pltpu.VMEM((n_dp, count, n_t, rows, 2 * units // n_t), BF16),
            pltpu.VMEM((n_dp, count, n_t, rows, 2 * units // n_t), BF16),
            pltpu.VMEM((n_dp, count, n_t, rows, units // n_t), BF16),
            pltpu.VMEM((count, rows, width), F32),
            pltpu.VMEM((n_dp - 1, count, rows, width), BF16),
            pltpu.VMEM((n_dp - 1, count, rows, width), BF16),
            pltpu.VMEM((count, rows, width), BF16),
            pltpu.VMEM((n_ex * parts, piece, width), BF16),
            pltpu.VMEM((tok, width), BF16),
            dma((5,)),
            dma,
            dma,
            dma,
            dma,
            dma((n_dp,)),
            dma,
            dma((n_ex * parts,)),
            dma,
            dma((n_dp - 1, count)),
            dma,
            dma((n_dp, count)),
            dma,
            dma((n_dp, count)),
            dma,
            dma((n_dp - 1, count)),
            dma,
            dma,
        ],
        compiler_params=pltpu.CompilerParams(
            collective_id=0, has_side_effects=True, vmem_limit_bytes=60 * 1024 * 1024
        ),
    )(tokens, ids, scores, weight_in, weight_out)


def solution(mesh):
    n_dp, n_ex, n_t = mesh.shape["dp"], mesh.shape["expert"], mesh.shape["tensor"]

    def whole(tokens, expert_ids, gate_scores, weight_in, weight_out):
        tok = tokens.shape[0] // (n_dp * n_ex)
        slots = min(3 * tok * expert_ids.shape[1] // (2 * n_ex), tok)
        group = max(1, n_ex // n_t)
        parts = 3 if group == 1 else 1
        cap = -(-slots // (16 * parts)) * 16 * parts
        return jax.shard_map(
            functools.partial(per_device, (n_dp, n_ex, n_t, cap, group, parts)),
            mesh=mesh,
            in_specs=(
                P(("dp", "expert"), "tensor"),
                P(None, ("dp", "expert")),
                P(None, ("dp", "expert")),
                P("expert", None, "tensor", "dp"),
                P("expert", "dp", "tensor"),
            ),
            out_specs=P(("dp", "expert"), "tensor"),
            check_vma=False,
        )(tokens, expert_ids.T, gate_scores.T, weight_in, weight_out)

    return whole
```

```python
import functools

import jax
import jax.numpy as jnp
from jax import lax
from jax.experimental import pallas as pl
from jax.experimental.pallas import tpu as pltpu
from jax.sharding import PartitionSpec as P

MESH = pl.DeviceIdType.MESH
F32 = jnp.float32
BF16 = jnp.bfloat16
SEND, FORWARD, PROJECT, ACTIVATE, EXPAND, COLLECT, NORMALIZE, SPREAD = range(8)
KINDS = "SFPAECNG"
TUNED = (
    "S032", "S012", "S010", "F000", "F002", "N000", "F032", "P032", "S021", "P002", "F001", "P000",
    "P001", "F012", "P102", "G000", "P132", "F010", "P010", "P012", "S022", "A001", "P101", "A032",
    "A132", "F021", "P021", "A002", "P100", "A012", "S031", "S030", "E132", "P112", "F022", "P121",
    "P110", "A021", "A112", "F031", "S020", "A121", "F030", "P031", "P122", "A000", "S011", "P022",
    "E121", "E032", "A010", "A102", "E112", "C032", "E012", "A122", "A110", "E021", "P131", "F020",
    "C021", "A022", "E122", "P130", "P030", "C012", "A131", "F011", "E022", "A101", "P011", "P120",
    "P020", "A100", "E110", "A130", "C022", "E131", "A120", "A030", "A031", "E010", "P111", "E130",
    "C010", "A011", "E031", "E120", "C031", "E000", "A020", "E030", "A111", "E100", "C030", "E001",
    "E020", "E111", "E102", "E002", "E011", "C020", "E101", "C011", "C000", "C001", "C002",
)


def dot(a, b):
    return jnp.dot(a, b, preferred_element_type=F32)


def lookup(values, index):
    base = 1 << max(values).bit_length()
    share = 1
    while base ** (share + 1) < 2**31:
        share += 1
    word = 0
    for i in range(0, len(values), share):
        packed = sum(v * base**k for k, v in enumerate(values[i : i + share]))
        word = jnp.where(index // share == i // share, packed, word)
    place, value = lax.rem(index, share), word
    for k in range(1, share):
        value = jnp.where(place == k, word // base**k, value)
    return lax.rem(value, base)


def make_plan(n_dp, chunks, parts):
    if (n_dp, chunks, parts) == (2, 4, 3):
        return [(KINDS.index(c[0]), *map(int, c[1:])) for c in TUNED]
    own = [(0, p) for p in range(parts)]
    offsets = sorted(range(1, chunks), key=lambda o: (o == 1, o))
    far = [(o, p) for o in offsets for p in range(parts)]
    units = own + far
    plan = []
    plan += [(SEND, 0, o, p) for o, p in far]
    for o, p in own:
        plan += [(FORWARD, 0, o, p)]
    count = len(units)
    plan += [(NORMALIZE, 0, 0, 0), (SPREAD, 0, 0, 0)]
    for s in range(count + 4):
        if parts <= s + 1 < count:
            plan.append((FORWARD, 0, *units[s + 1]))
        for kind in (PROJECT, ACTIVATE, EXPAND):
            if s < count:
                plan.append((kind, 0, *units[s]))
            if 0 <= s - 1 < count:
                plan += [(kind, h, *units[s - 1]) for h in range(1, n_dp)]
        if 0 <= s - 3 < count:
            plan.append((COLLECT, 0, *units[s - 3]))
    return plan


def kernel(
    sizes,
    plan,
    tokens_hbm,
    ids_hbm,
    scores_hbm,
    w_in_hbm,
    w_out_hbm,
    mixed,
    tokens,
    ids,
    scores,
    w_in,
    w_out,
    slot_t,
    squares,
    scale_out,
    scales_in,
    outgoing,
    rows_in,
    part,
    part_in,
    hidden,
    keep,
    down,
    down_in,
    home,
    home_in,
    result,
    combine,
    local_sem,
    sq,
    rq,
    sn,
    sm,
    rn,
    sz,
    rz,
    sx,
    rx,
    sp,
    rp,
    sh,
    rh,
    so,
    ro,
    sr,
    rr,
):
    n_dp, n_ex, n_t, cap, group, parts = sizes
    d, e, t = lax.axis_index("dp"), lax.axis_index("expert"), lax.axis_index("tensor")
    chunks = n_ex // group
    piece = cap // parts
    ec, ei = e // group, lax.rem(e, group)
    tok, width = tokens.shape
    top = ids.shape[0]
    units = w_out.shape[0]
    sub = units // n_t
    rows = group * piece
    width_all = width * n_t

    def at(index, step, count):
        return lax.rem(index + step + count, count)

    def copy(src, dst, send, recv, **index):
        return pltpu.make_async_remote_copy(
            src_ref=src, dst_ref=dst, send_sem=send, recv_sem=recv,
            device_id=index, device_id_type=MESH,
        )

    def pending(like, sem):
        return pltpu.make_async_copy(like, like, sem)

    load_tokens = pltpu.make_async_copy(tokens_hbm, tokens, local_sem.at[0])
    load_in = pltpu.make_async_copy(w_in_hbm.at[0], w_in, local_sem.at[1])
    load_out = pltpu.make_async_copy(w_out_hbm.at[0], w_out, local_sem.at[2])
    load_ids = pltpu.make_async_copy(ids_hbm, ids, local_sem.at[3])
    load_scores = pltpu.make_async_copy(scores_hbm, scores, local_sem.at[4])
    load_ids.start()
    load_tokens.start()
    barrier = pltpu.get_barrier_semaphore()
    for axis, me, count in (("expert", e, n_ex), ("dp", d, n_dp), ("tensor", t, n_t)):
        for step in range(1, count):
            pl.semaphore_signal(
                barrier, inc=1, device_id={axis: at(me, step, count)}, device_id_type=MESH
            )
    load_scores.start()
    load_in.start()
    load_out.start()

    tok_rows = lax.broadcasted_iota(jnp.int32, (tok, tok), 0)
    tok_lanes = lax.broadcasted_iota(jnp.int32, (tok, tok), 1)
    wide_ex = max(128, n_ex)
    ex_rows = lax.broadcasted_iota(jnp.int32, (wide_ex, tok), 0)
    named_t = ex_rows < 0
    load_ids.wait()
    for k in range(top):
        named_t = named_t | (ex_rows == ids[k : k + 1, :])
    count_t = dot(named_t.astype(F32).astype(BF16), (tok_rows < tok_lanes).astype(F32).astype(BF16))
    slot_t[...] = jnp.where(named_t, count_t, -1.0)

    def block(ref, lead, member, p):
        u = (member // group) * parts + p
        if group == 1:
            return ref.at[(*lead, u)]
        return ref.at[(*lead, u, pl.ds(pl.multiple_of(lax.rem(member, group) * piece, piece), piece))]

    def z_copy(expert, p):
        return copy(
            outgoing.at[expert * parts + p], block(rows_in, (0,), e, p),
            sz, rz.at[e * parts + p], expert=expert,
        )

    def z_wait(source, p):
        copy(
            outgoing.at[source * parts + p], block(rows_in, (0,), source, p),
            sz, rz.at[source * parts + p], expert=source,
        ).wait_recv()

    def x_copy(u, hop):
        return copy(
            rows_in.at[0, u], rows_in.at[n_dp - hop, u],
            sx, rx.at[n_dp - hop - 1, u], dp=at(d, hop, n_dp),
        )

    def part_copy(h, u, step):
        to = at(t, step, n_t)
        return copy(part.at[h, u, to], part_in.at[h, u, t], sp, rp.at[h, u], tensor=to)

    def hidden_copy(h, u, step):
        to = at(t, step, n_t)
        return copy(hidden.at[h, u, t], hidden.at[h, u, t], sh, rh.at[h, u], tensor=to)

    def down_copy(h, u):
        return copy(
            down.at[h - 1, u], down_in.at[n_dp - h - 1, u], so, ro.at[n_dp - h - 1, u], dp=at(d, h, n_dp)
        )

    def home_copy(expert, p):
        return copy(
            block(home, (), expert, p), home_in.at[e * parts + p],
            sr, rr, expert=expert,
        )

    piece_rows = lax.broadcasted_iota(jnp.int32, (piece, tok), 0)
    diagonal = piece_rows == lax.broadcasted_iota(jnp.int32, (piece, tok), 1)

    def picked(expert, p):
        want = (piece_rows + p * piece).astype(F32)
        return want == slot_t[expert : expert + 1, :]

    with SCOPE("tok"):
        load_tokens.wait()
    for expert in range(n_ex):
        pick = jnp.concatenate([picked(expert, p).astype(F32) for p in range(parts)], axis=0).astype(BF16)
        outgoing[expert * parts : (expert + 1) * parts] = (
            dot(pick, tokens[...]).astype(BF16).reshape(parts, piece, width)
        )
    for p in range(parts):
        block(rows_in, (0,), e, p)[...] = outgoing[e * parts + p]
    wide = tokens[...].astype(F32)
    own_squares = jnp.sum(wide * wide, axis=1, keepdims=True)
    own_squares = jnp.sum(jnp.where(tok_rows == tok_lanes, own_squares, 0.0), axis=0, keepdims=True)
    squares[t] = jnp.broadcast_to(own_squares, (8, tok))
    with SCOPE("barrier"):
        pl.semaphore_wait(barrier, n_dp + n_ex + n_t - 3)
    for step in range(1, n_t):
        copy(squares.at[t], squares.at[t], sq, rq, tensor=at(t, step, n_t)).start()

    def normalize():
        pending(squares.at[: n_t - 1], rq).wait()
        total = squares[0, 0:1, :]
        for s in range(1, n_t):
            total = total + squares[s, 0:1, :]
        scale = lax.rsqrt(total / width_all + 1e-06)
        tile_rows = lax.broadcasted_iota(jnp.int32, (8, tok), 0)
        for expert in range(n_ex):
            tile = jnp.zeros((8, tok), F32)
            for p in range(parts):
                column = jnp.sum(jnp.where(picked(expert, p), scale, 0.0), axis=1, keepdims=True)
                row = jnp.sum(jnp.where(diagonal, column, 0.0), axis=0, keepdims=True)
                tile = jnp.where(tile_rows == p, row, tile)
            scale_out[expert] = tile
        scales_in[0, e] = scale_out[e]
        for step in range(1, n_ex):
            to = at(e, step, n_ex)
            copy(scale_out.at[to], scales_in.at[0, e], sn, rn.at[0], expert=to).start()

    def weigh():
        load_scores.wait()
        weights = []
        for expert in range(n_ex):
            score = jnp.zeros((1, tok), F32)
            for k in range(top):
                score = score + jnp.where(ids[k : k + 1, :] == expert, scores[k : k + 1, :].astype(F32), 0.0)
            weights += [jnp.where(picked(expert, p), score, 0.0) for p in range(parts)]
        combine[...] = jnp.transpose(jnp.concatenate(weights, axis=0)).astype(BF16)

    def spread():
        pending(scales_in.at[0, : n_ex - 1], rn.at[0]).wait()
        for hop in range(1, n_dp):
            copy(scales_in.at[0], scales_in.at[n_dp - hop], sm, rn.at[n_dp - hop], dp=at(d, hop, n_dp)).start()

    def send(q, p):
        for i in range(group):
            expert = q * group + i

            @pl.when(expert != e)
            def _():
                z_copy(expert, p).start()

    def forward(q, p):
        for i in range(group):
            source = q * group + i

            @pl.when(source != e)
            def _():
                z_wait(source, p)

        for hop in range(1, n_dp):
            x_copy(q * parts + p, hop).start()

    def project(h, u):
        @pl.when(h > 0)
        def _():
            copy(rows_in.at[0, u], rows_in.at[h, u], sx, rx.at[h - 1, u], dp=at(d, h, n_dp)).wait_recv()

        block_rows = rows_in[h, u]
        for g in range(2):
            sums = dot(block_rows, w_in[g]).astype(BF16)
            for to in range(n_t):
                part[h, u, to, :, g * sub : (g + 1) * sub] = sums[:, to * sub : (to + 1) * sub]
        for step in range(1, n_t):
            part_copy(h, u, step).start()

    def activate(h, q, p):
        u = q * parts + p
        pending(part_in.at[h, u, : n_t - 1], rp.at[h, u]).wait()
        total = part[h, u, t].astype(F32)
        for step in range(1, n_t):
            total = total + part_in[h, u, at(t, step, n_t)].astype(F32)
        scale = [
            jnp.sum(
                jnp.where(diagonal, scales_in[h, q * group + i, pl.ds(p, 1), :], 0.0), axis=1, keepdims=True
            )
            for i in range(group)
        ]
        total = total * jnp.concatenate(scale, axis=0)
        gate, up = total[:, :sub], total[:, sub:]
        hidden[h, u, t] = (gate / (1.0 + jnp.exp(-gate)) * up).astype(BF16)
        for step in range(1, n_t):
            hidden_copy(h, u, step).start()

    def expand(h, u):
        pending(hidden.at[h, u, : n_t - 1], rh.at[h, u]).wait()
        full = jnp.concatenate([hidden[h, u, s] for s in range(n_t)], axis=1)
        result = dot(full, w_out[...])

        @pl.when(h == 0)
        def _():
            keep[u] = result

        @pl.when(h > 0)
        def _():
            down[h - 1, u] = result.astype(BF16)
            down_copy(h, u).start()

    def collect(q, p):
        u = q * parts + p
        total = keep[u]
        for h in range(1, n_dp):
            copy(
                down.at[h - 1, u], down_in.at[h - 1, u], so, ro.at[h - 1, u], dp=at(d, h, n_dp)
            ).wait_recv()
            total = total + down_in[h - 1, u].astype(F32)
        home[u] = total.astype(BF16)
        for i in range(group):
            expert = q * group + i

            @pl.when(expert != e)
            def _():
                home_copy(expert, p).start()

            @pl.when(expert == e)
            def _():
                home_in[expert * parts + p] = home[u, i * piece : (i + 1) * piece]

    first_project = min(i for i, op in enumerate(plan) if op[0] == PROJECT)
    first_far = [min(i for i, op in enumerate(plan) if op[:2] == (ACTIVATE, h)) for h in range(1, n_dp)]
    first_expand = min(i for i, op in enumerate(plan) if op[0] == EXPAND)

    codes = [kind + 8 * (h + n_dp * (p + parts * o)) for kind, h, o, p in plan]

    @pl.loop(0, len(plan))
    def _(step):
        code = lookup(codes, step)
        kind, rest = lax.rem(code, 8), code // 8
        h, rest = lax.rem(rest, n_dp), rest // n_dp
        p, o = lax.rem(rest, parts), rest // parts
        to, q = lax.rem(ec + o, chunks), lax.rem(ec - o + chunks, chunks)
        u = q * parts + p

        @pl.when(kind == SEND)
        def _():
            with SCOPE("send"):
                send(to, p)

        @pl.when(kind == FORWARD)
        def _():
            with SCOPE("forward"):
                forward(q, p)

        @pl.when(kind == PROJECT)
        def _():
            @pl.when(step == first_project)
            def _():
                load_in.wait()

            with SCOPE("project"):
                project(h, u)

        @pl.when(kind == ACTIVATE)
        def _():
            for hop in range(1, n_dp):
                @pl.when(step == first_far[hop - 1])
                def _():
                    pending(scales_in.at[hop], rn.at[hop]).wait()

            with SCOPE("activate"):
                activate(h, q, p)

        @pl.when(kind == EXPAND)
        def _():
            @pl.when(step == first_expand)
            def _():
                load_out.wait()

            with SCOPE("expand"):
                expand(h, u)

        @pl.when(kind == NORMALIZE)
        def _():
            with SCOPE("normalize"):
                normalize()

        @pl.when(kind == SPREAD)
        def _():
            with SCOPE("weigh"):
                weigh()

            with SCOPE("spread"):
                spread()

        @pl.when(kind == COLLECT)
        def _():
            with SCOPE("collect"):
                collect(q, p)

    others = (n_ex - 1) * parts
    with SCOPE("homes"):
        pending(home_in.at[:others], rr).wait()

    stores = []
    with SCOPE("mix"):
        for i, start in enumerate(range(0, width, width // 2)):
            columns = slice(start, start + width // 2)
            result[:, columns] = dot(combine[...], home_in[:, :, columns].reshape(n_ex * cap, width // 2)).astype(BF16)
            stores.append(pltpu.make_async_copy(result.at[:, columns], mixed.at[:, columns], local_sem.at[i]))
            stores[i].start()

    with SCOPE("drain"):
        pending(squares.at[: n_t - 1], sq).wait()
        pending(scales_in.at[0, : n_ex - 1], sn).wait()
        pending(scales_in.at[1:], sm).wait()
        pending(outgoing.at[:others], sz).wait()
        pending(home_in.at[:others], sr).wait()
        pending(down, so).wait()
        pending(rows_in.at[1:], sx).wait()
        pending(part.at[:, :, : n_t - 1], sp).wait()
        pending(hidden.at[:, :, : n_t - 1], sh).wait()
        for store in stores:
            store.wait()


SCOPE = jax.named_scope


def per_device(sizes, tokens, ids, scores, weight_in, weight_out):
    n_dp, n_ex, n_t, cap, group, parts = sizes
    tok, width = tokens.shape
    units = weight_out.shape[1]
    chunks = n_ex // group
    count = chunks * parts
    piece = cap // parts
    rows = group * piece
    plan = make_plan(n_dp, chunks, parts)
    dma = pltpu.SemaphoreType.DMA
    top = ids.shape[0]
    hbm = pl.BlockSpec(memory_space=pl.ANY)
    return pl.pallas_call(
        functools.partial(kernel, sizes, plan),
        out_shape=jax.ShapeDtypeStruct((tok, width), BF16),
        in_specs=[hbm] * 5,
        out_specs=hbm,
        scratch_shapes=[
            pltpu.VMEM((tok, width), BF16),
            pltpu.VMEM((top, tok), jnp.int32),
            pltpu.VMEM((top, tok), BF16),
            pltpu.VMEM((2, width, units), BF16),
            pltpu.VMEM((units, width), BF16),
            pltpu.VMEM((max(128, n_ex), tok), F32),
            pltpu.VMEM((n_t, 8, tok), F32),
            pltpu.VMEM((n_ex, 8, tok), F32),
            pltpu.VMEM((n_dp, n_ex, 8, tok), F32),
            pltpu.VMEM((n_ex * parts, piece, width), BF16),
            pltpu.VMEM((n_dp, count, rows, width), BF16),
            pltpu.VMEM((n_dp, count, n_t, rows, 2 * units // n_t), BF16),
            pltpu.VMEM((n_dp, count, n_t, rows, 2 * units // n_t), BF16),
            pltpu.VMEM((n_dp, count, n_t, rows, units // n_t), BF16),
            pltpu.VMEM((count, rows, width), F32),
            pltpu.VMEM((n_dp - 1, count, rows, width), BF16),
            pltpu.VMEM((n_dp - 1, count, rows, width), BF16),
            pltpu.VMEM((count, rows, width), BF16),
            pltpu.VMEM((n_ex * parts, piece, width), BF16),
            pltpu.VMEM((tok, width), BF16),
            pltpu.VMEM((tok, n_ex * cap), BF16),
            dma((5,)),
            dma,
            dma,
            dma,
            dma,
            dma((n_dp,)),
            dma,
            dma((n_ex * parts,)),
            dma,
            dma((n_dp - 1, count)),
            dma,
            dma((n_dp, count)),
            dma,
            dma((n_dp, count)),
            dma,
            dma((n_dp - 1, count)),
            dma,
            dma,
        ],
        compiler_params=pltpu.CompilerParams(
            collective_id=0, has_side_effects=True, vmem_limit_bytes=60 * 1024 * 1024
        ),
    )(tokens, ids, scores, weight_in, weight_out)


def solution(mesh):
    n_dp, n_ex, n_t = mesh.shape["dp"], mesh.shape["expert"], mesh.shape["tensor"]

    def whole(tokens, expert_ids, gate_scores, weight_in, weight_out):
        tok = tokens.shape[0] // (n_dp * n_ex)
        slots = min(3 * tok * expert_ids.shape[1] // (2 * n_ex), tok)
        group = max(1, n_ex // n_t)
        parts = 3 if group == 1 else 1
        cap = -(-slots // (16 * parts)) * 16 * parts
        return jax.shard_map(
            functools.partial(per_device, (n_dp, n_ex, n_t, cap, group, parts)),
            mesh=mesh,
            in_specs=(
                P(("dp", "expert"), "tensor"),
                P(None, ("dp", "expert")),
                P(None, ("dp", "expert")),
                P("expert", None, "tensor", "dp"),
                P("expert", "dp", "tensor"),
            ),
            out_specs=P(("dp", "expert"), "tensor"),
            check_vma=False,
        )(tokens, expert_ids.T, gate_scores.T, weight_in, weight_out)

    return whole
```
